32 devices in a mesh: gx: 4 (over y, x), gy: 4 (over z), gz: 2 (over core).
Axes of the slice: x: 2, y: 2, z: 4, core: 2. Of those that a mesh axis runs over, the one named last changes fastest.
Arguments:
- rhs: bfloat16 [2, 4096, 4096], P('gz', 'gx', 'gy'), may hold values from -40 to 40
- basis_x: bfloat16 [4096, 4096], P('gx', ('gy', 'gz')), may hold values from -0.125 to 0.125
- basis_y: bfloat16 [4096, 4096], P('gy', ('gx', 'gz')), may hold values from -0.125 to 0.125
- eig_x: float32 [4096], P('gx'), may hold values from 0.1 to 4
- eig_y: float32 [4096], P('gy'), may hold values from 0.1 to 4
- eig_z: float32 [2], P('gz'), may hold values from 0.1 to 4
Outputs:
- solution: bfloat16 [2, 4096, 4096], P('gz', 'gx', 'gy')
- energy: float32 [], replicated
The draws below stay inside these ranges and needn't reach their ends.
All inputs are finite; a program needn't handle non-finite values.
Results may differ from the reference program's by a relative error of at most 0.01.
Values may be sent and summed in bfloat16 or wider, within the bound.
A program may use at most 128 MiB of HBM per device.

```python
import math
import jax
import jax.numpy as jnp

NX = 4096
NY = 4096
KZ = 2


def draw_rhs(key, part):
    first_key, second_key = jax.random.split(jax.random.fold_in(key, 17))
    position = jnp.arange(NX, dtype=jnp.float32) / NX
    rough = jnp.exp(jax.random.uniform(second_key, (NX,), jnp.float32, -0.7, 0.7))
    values = jnp.clip(jax.random.normal(first_key, (KZ, NX, NY), jnp.float32), -6.0, 6.0)
    trend = jnp.exp(jnp.log(3.0) * position)
    return (values * (trend * rough)[None, :, None]).astype(jnp.bfloat16)


def with_spikes(drawn, key, source, target, shards_of, factor):
    owner, partner = [(jnp.arange(drawn.shape[dim]) // (drawn.shape[dim] // shards_of)).reshape([-1 if axis == dim else 1 for axis in range(drawn.ndim)]) for dim in (source, target)]
    chosen = jax.random.permutation(key, shards_of)[partner]
    strong = (owner == chosen) | (owner == (partner + shards_of // 2) % shards_of)
    return jnp.where(strong, factor * drawn, drawn)


def levels(own_key, extent, shards, smallest, largest):
    gain = 1.0
    for dim, shards_of in shards:
        heights = jax.random.uniform(jax.random.fold_in(jax.random.fold_in(own_key, 6), dim), (shards_of,), jnp.float32, smallest / len(shards), largest / len(shards))
        gain = gain * jnp.repeat(jnp.exp(heights), extent[dim] // shards_of).reshape((-1,) + (1,) * (len(extent) - 1 - dim))
    return gain


def gaussian_with(key, extent, spread, bound, cuts, heavy, held_as=jnp.bfloat16):
    array = spread * jax.random.normal(key, extent, jnp.float32)
    if cuts:
        array = array * levels(key, extent, cuts, -0.22, 0.18)
    return jnp.clip(with_spikes(array, jax.random.fold_in(key, 3), *heavy), -bound, bound).astype(held_as)


def setup_inputs(seed: int = 0) -> dict:
    arg_keys = jax.random.split(jax.random.key(seed), 7)
    return {
        "rhs": draw_rhs(jax.random.fold_in(arg_keys[6], 71), 0),
        "basis_x": gaussian_with(arg_keys[1], (NX, NX), NX ** -0.5, 0.125, ((0, 4), (1, 8)), (0, 1, 8, 2.0)),
        "basis_y": gaussian_with(arg_keys[2], (NY, NY), NY ** -0.5, 0.125, ((0, 4), (1, 8)), (0, 1, 8, 2.0)),
        "eig_x": jnp.clip(jnp.exp(math.log(4.0) - 3.6888794 * jax.random.uniform(arg_keys[3], (NX,), jnp.float32) ** levels(arg_keys[3], (NX,), ((0, 4),), -0.2, 0.2)), 0.1, 4.0),
        "eig_y": jnp.clip(jnp.exp(math.log(4.0) - 3.6888794 * jax.random.uniform(arg_keys[4], (NY,), jnp.float32) ** levels(arg_keys[4], (NY,), ((0, 4),), -0.2, 0.2)), 0.1, 4.0),
        "eig_z": jnp.clip(jnp.exp(math.log(4.0) - 3.6888794 * jax.random.uniform(arg_keys[5], (KZ,), jnp.float32) ** levels(arg_keys[5], (KZ,), ((0, 2),), -0.2, 0.2)), 0.1, 4.0),
    }


def reference(rhs, basis_x, basis_y, eig_x, eig_y, eig_z):
    basis_xf = basis_x.astype(jnp.float32)
    basis_yf = basis_y.astype(jnp.float32)
    rhs_wide = rhs.astype(jnp.float32)
    section_g = jnp.einsum('xi,kxy->kiy', basis_xf, rhs_wide).astype(jnp.bfloat16)
    section_h = jnp.einsum('yj,kiy->kij', basis_yf, section_g.astype(jnp.float32))
    denominator = eig_z[:, None, None] + eig_x[None, :, None] + eig_y[None, None, :]
    scaled = (section_h / denominator).astype(jnp.bfloat16)
    section_v = jnp.einsum('yj,kij->kiy', basis_yf, scaled.astype(jnp.float32)).astype(jnp.bfloat16)
    section_s = jnp.einsum('xi,kiy->kxy', basis_xf, section_v.astype(jnp.float32))
    return section_s.astype(jnp.bfloat16), jnp.sum(rhs_wide * section_s)
```

```python
import functools

import jax
import jax.numpy as jnp
from jax import lax
from jax.sharding import PartitionSpec as P

CHUNKS = 2


def dot(spec, left, right):
    return jnp.einsum(spec, left, right, preferred_element_type=jnp.float32)


def shards(nx, ny, rhs, basis_x, basis_y, eig_x, eig_y, eig_z):
    bf16 = jnp.bfloat16
    panel_x = lax.all_gather(basis_x, ("gy", "gz"), axis=1, tiled=True)
    panel_y = lax.all_gather(basis_y, ("gx", "gz"), axis=1, tiled=True)
    me_x, me_y = lax.axis_index("gx"), lax.axis_index("gy")
    block_i, block_j = panel_x.shape[1] // nx, panel_y.shape[1] // ny
    width = block_i // CHUNKS
    others = sorted(range(1, nx), key=lambda d: -bin(d).count("1"))

    def columns_x(distance, chunk):
        return lax.dynamic_slice_in_dim(panel_x, (me_x ^ distance) * block_i + chunk * width, width, axis=1)

    def columns_y(offset):
        start = jnp.clip(me_y + offset, 0, ny - 1) * block_j
        return lax.dynamic_slice_in_dim(panel_y, start, block_j, axis=1)

    def swap_x(value, distance):
        return lax.ppermute(value, "gx", [(a, a ^ distance) for a in range(nx)])

    def forward_x(values, chunk):
        sent = [swap_x(dot("xi,xy->iy", columns_x(d, chunk), values).astype(bf16), d) for d in others]
        total = dot("xi,xy->iy", columns_x(0, chunk), values)
        for piece in sent:
            total = total + piece.astype(jnp.float32)
        return total.astype(bf16)

    def forward_y(section):
        total = None
        up, down = None, None
        for tick in range(1, ny):
            ahead = dot("yj,iy->ji", columns_y(ny - tick), section)
            behind = dot("yj,iy->ji", columns_y(tick - ny), section)
            if up is not None:
                ahead = ahead + up.astype(jnp.float32)
                behind = behind + down.astype(jnp.float32)
            up = lax.ppermute(ahead.astype(bf16), "gy", [(b, b + 1) for b in range(tick)])
            down = lax.ppermute(behind.astype(bf16), "gy", [(ny - 1 - b, ny - 2 - b) for b in range(tick)])
        total = dot("yj,iy->ji", columns_y(0), section)
        if up is not None:
            total = total + up.astype(jnp.float32) + down.astype(jnp.float32)
        return total

    energy = jnp.float32(0)
    solved = []
    for k in range(rhs.shape[0]):
        sections = [forward_x(rhs[k], chunk) for chunk in range(CHUNKS)]
        scaled = []
        for chunk, section in enumerate(sections):
            h = forward_y(section)
            w = h / (eig_x[chunk * width : (chunk + 1) * width][None, :] + eig_y[:, None] + eig_z[k])
            w, part = lax.optimization_barrier((w.astype(bf16), jnp.sum(h * w)))
            energy = energy + part
            scaled.append(w)
        s = None
        for chunk, w in enumerate(scaled):
            v = dot("yj,ji->iy", panel_y, lax.all_gather(w, "gy", axis=0, tiled=True)).astype(bf16)
            for d in others + [0]:
                piece = v if d == 0 else swap_x(v, d)
                term = dot("xi,iy->xy", columns_x(d, chunk), piece)
                s = term if s is None else s + term
        solved.append(s.astype(bf16))
    return jnp.stack(solved), lax.psum(energy, ("gx", "gy", "gz"))


def solution(mesh):
    return jax.shard_map(
        functools.partial(shards, mesh.shape["gx"], mesh.shape["gy"]),
        mesh=mesh,
        in_specs=(
            P("gz", "gx", "gy"),
            P("gx", ("gy", "gz")),
            P("gy", ("gx", "gz")),
            P("gx"),
            P("gy"),
            P("gz"),
        ),
        out_specs=(P("gz", "gx", "gy"), P()),
        check_vma=False,
    )
```
